32 devices in a mesh: gx: 4 (over z), gy: 2 (over x), gz: 4 (over y, core).
Axes of the slice: x: 2, y: 2, z: 4, core: 2. Of those that a mesh axis runs over, the one named last changes fastest.
Arguments:
- constraint: bfloat16 [4, 2, 4, 256, 3072], P('gx', 'gy', 'gz'), may hold values from -1.5 to 1.5
- stiff_ib: bfloat16 [4, 2, 4, 256, 3072], P('gx', 'gy', 'gz'), may hold values from -0.75 to 0.75
- mass_ib: bfloat16 [4, 2, 4, 256, 3072], P('gx', 'gy', 'gz'), may hold values from -1.5 to 1.5
- mass_ii: float32 [4, 2, 4, 256], P('gx', 'gy', 'gz'), may hold values from 0.5 to 4
- modes: bfloat16 [4, 2, 4, 300, 256], P('gx', 'gy', 'gz'), may hold values from -0.375 to 0.375
- stiff_faces: bfloat16 [4, 2, 4, 6, 512, 512], P('gx', 'gy', 'gz'), may hold values from -3 to 3
- mass_faces: bfloat16 [4, 2, 4, 6, 512], P('gx', 'gy', 'gz'), may hold values from 0.19921875 to 4
- dof_map: int32 [4, 2, 4, 3, 512], P('gx', 'gy', 'gz'), may hold values from 0 to 511, each once within a row
Outputs:
- stiff_assembled: bfloat16 [4, 2, 4, 3, 512, 512], P('gx', 'gy', 'gz')
- mass_assembled: bfloat16 [4, 2, 4, 3, 512, 512], P('gx', 'gy', 'gz')
- modal_coupling: bfloat16 [4, 2, 4, 3, 600, 512], P('gx', 'gy', 'gz')
The draws below stay inside these ranges and needn't reach their ends.
Inputs may be any that keep to these rules, and one draw needn't show every extreme that they name: `dof_map`: each row of the last dimension is a permutation of 0 to 511.
All inputs are finite; a program needn't handle non-finite values.
Results may differ from the reference program's by a relative error of at most 0.0075.
Values may be sent and summed in bfloat16 or wider, within the bound.
No kernel may reach another device: no remote copies, remote signals or barrier semaphores. Data moves between devices by JAX's collectives and lax.ppermute only.
A program may use at most 64 MiB of HBM per device.

```python
import math
import jax
import jax.numpy as jnp
from jax import lax

FACE = 512
MODES = 300
NI = 256
B = 3072
N_GX = 4
N_GY = 2
N_GZ = 4


def block_levels(key, dims, split, smallest, top_value):
    def one(axis_at, shards_of):
        heights = jax.random.uniform(jax.random.fold_in(jax.random.fold_in(key, 6), axis_at), (shards_of,), jnp.float32, smallest / len(split), top_value / len(split))
        return jnp.repeat(jnp.exp(heights), dims[axis_at] // shards_of).reshape((-1,) + (1,) * (len(dims) - axis_at - 1))

    level = one(*split[0])
    for cut in split[1:]:
        level = level * one(*cut)
    return level


def centred(key, dims, scale, bound, shards=(), held_as=jnp.bfloat16):
    array = scale * jax.random.normal(key, dims, jnp.float32)
    if shards:
        array = array * block_levels(key, dims, shards, -0.22, 0.18)
    return jnp.clip(array, -bound, bound).astype(held_as)


def setup_inputs(seed: int = 0) -> dict:
    key_of = jax.random.split(jax.random.key(seed), 9)
    constraint = centred(key_of[0], (N_GX, N_GY, N_GZ, NI, B), 0.25, 1.5, ((0, 4), (1, 2), (2, 4)))
    stiff_ib = centred(key_of[1], (N_GX, N_GY, N_GZ, NI, B), (NI // 4) ** -0.5, 0.75, ((0, 4), (1, 2), (2, 4)))
    mass_ib = centred(key_of[2], (N_GX, N_GY, N_GZ, NI, B), 0.25, 1.5, ((0, 4), (1, 2), (2, 4)))
    mass_ii = jnp.clip(jnp.exp(math.log(4.0) - 2.0794415 * jax.random.uniform(key_of[3], (N_GX, N_GY, N_GZ, NI), jnp.float32) ** block_levels(key_of[3], (N_GX, N_GY, N_GZ, NI), ((0, 4), (1, 2), (2, 4)), -0.2, 0.2)), 0.5, 4.0)
    modes = centred(key_of[4], (N_GX, N_GY, N_GZ, MODES, NI), NI ** -0.5, 0.375, ((0, 4), (1, 2), (2, 4)))
    stiff_faces = centred(key_of[5], (N_GX, N_GY, N_GZ, 6, FACE, FACE), 0.5, 3.0, ((0, 4), (1, 2), (2, 4)))
    mass_faces = jnp.clip(jnp.exp(math.log(4.0) - 2.9996462 * jax.random.uniform(key_of[6], (N_GX, N_GY, N_GZ, 6, FACE), jnp.float32) ** block_levels(key_of[6], (N_GX, N_GY, N_GZ, 6, FACE), ((0, 4), (1, 2), (2, 4)), -0.2, 0.2)), 0.19921875, 4.0).astype(jnp.bfloat16)
    dof_map = jax.vmap(lambda own: jax.random.permutation(own, FACE))(jax.random.split(key_of[7], N_GX * N_GY * N_GZ * 3)).reshape((N_GX, N_GY, N_GZ, 3, FACE)).astype(jnp.int32)
    return dict(constraint=constraint, stiff_ib=stiff_ib, mass_ib=mass_ib, mass_ii=mass_ii, modes=modes, stiff_faces=stiff_faces, mass_faces=mass_faces, dof_map=dof_map)


def transposed(left, right):
    return lax.dot_general(left, right, (((0,), (0,)), ((), ())), preferred_element_type=jnp.float32)


def superelement(items):
    constraint, stiff_ib, mass_ib, mass_ii, modes, stiff_faces, mass_faces = items
    loaded = (mass_ib.astype(jnp.float32) + mass_ii[:, None] * constraint.astype(jnp.float32)).astype(jnp.bfloat16)
    coupling = jnp.dot(modes, loaded, preferred_element_type=jnp.float32).astype(jnp.bfloat16)
    width = stiff_faces.shape[-1]
    stiff_list = []
    mass_list = []
    for face in range(6):
        lower = face * width
        stiff_cols = stiff_ib[:, lower:lower + width]
        mass_cols = mass_ib[:, lower:lower + width]
        cons_cols = constraint[:, lower:lower + width]
        load_cols = loaded[:, lower:lower + width]
        stiff_list.append((stiff_faces[face].astype(jnp.float32) + transposed(stiff_cols, cons_cols)).astype(jnp.bfloat16))
        mass_list.append((jnp.diag(mass_faces[face].astype(jnp.float32)) + transposed(cons_cols, load_cols) + transposed(mass_cols, cons_cols)).astype(jnp.bfloat16))
    return jnp.stack(stiff_list), jnp.stack(mass_list), coupling


def upper_neighbour(values, axis):
    size = values.shape[axis]
    rest = lax.slice_in_dim(values, 1, size, axis=axis)
    pad = jnp.zeros_like(lax.slice_in_dim(values, 0, 1, axis=axis))
    return jnp.concatenate([rest, pad], axis=axis)


def reference(constraint, stiff_ib, mass_ib, mass_ii, modes, stiff_faces, mass_faces, dof_map):
    grid = constraint.shape[:3]
    count = grid[0] * grid[1] * grid[2]
    items = tuple(a.reshape((count,) + a.shape[3:]) for a in (constraint, stiff_ib, mass_ib, mass_ii, modes, stiff_faces, mass_faces))
    stiff_red, mass_red, coupling = lax.map(superelement, items)
    stiff_red = stiff_red.reshape(grid + stiff_red.shape[1:])
    mass_red = mass_red.reshape(grid + mass_red.shape[1:])
    coupling = coupling.reshape(grid + coupling.shape[1:])
    width = stiff_red.shape[-1]
    stiff_out = []
    mass_out = []
    coup_out = []
    for axis in range(3):
        mapping = dof_map[:, :, :, axis, :].astype(jnp.int32)
        high = 2 * axis + 1
        low = 2 * axis
        stiff_nb = upper_neighbour(stiff_red[:, :, :, low], axis)
        mass_nb = upper_neighbour(mass_red[:, :, :, low], axis)
        coup_nb = upper_neighbour(coupling[:, :, :, :, low * width:(low + 1) * width], axis)
        rows = mapping[:, :, :, :, None]
        cols = mapping[:, :, :, None, :]
        stiff_nb = jnp.take_along_axis(jnp.take_along_axis(stiff_nb, rows, axis=3), cols, axis=4)
        mass_nb = jnp.take_along_axis(jnp.take_along_axis(mass_nb, rows, axis=3), cols, axis=4)
        coup_nb = jnp.take_along_axis(coup_nb, cols, axis=4)
        stiff_out.append((stiff_red[:, :, :, high].astype(jnp.float32) + stiff_nb.astype(jnp.float32)).astype(jnp.bfloat16))
        mass_out.append((mass_red[:, :, :, high].astype(jnp.float32) + mass_nb.astype(jnp.float32)).astype(jnp.bfloat16))
        coup_out.append(jnp.concatenate([coupling[:, :, :, :, high * width:(high + 1) * width], coup_nb], axis=3))
    return jnp.stack(stiff_out, axis=3), jnp.stack(mass_out, axis=3), jnp.stack(coup_out, axis=3)
```

```python
import functools

import jax
import jax.numpy as jnp
from jax import lax
from jax.experimental import pallas as pl
from jax.experimental.pallas import tpu as pltpu
from jax.sharding import PartitionSpec as P


F32 = jnp.float32
BF16 = jnp.bfloat16


def shifted(block, axis):
    size = lax.axis_size(axis)
    return lax.ppermute(block, axis, [(i, i - 1) for i in range(1, size)])


def dot(left, right, over):
    return lax.dot_general(left, right, ((over[:1], over[1:]), ((), ())), preferred_element_type=F32)


def column(row, lanes=128):
    return jnp.transpose(jnp.broadcast_to(row, (lanes, row.shape[1])))


def across(col, width):
    return jnp.concatenate([col] * (width // col.shape[1]), axis=1)


def stiff_of(stiff, cons, face):
    return (face.astype(F32) + dot(stiff, cons, (0, 0))).astype(BF16)


def loaded_of(mass, cons, lumped):
    scale = across(column(lumped), cons.shape[1])
    return (mass.astype(F32) + scale * cons.astype(F32)).astype(BF16)


def diagonal(shape):
    return lax.broadcasted_iota(jnp.int32, shape, 0) == lax.broadcasted_iota(jnp.int32, shape, 1)


def low_stiff_kernel(stiff_ref, cons_ref, face_ref, out_ref):
    out_ref[...] = stiff_of(stiff_ref[...], cons_ref[...], face_ref[0])


def low_mass_kernel(cons_ref, mass_ref, lumped_ref, modes_ref, diag_ref, out_ref):
    cons = cons_ref[...]
    mass = mass_ref[...]
    half = cons.shape[1] // 2
    load = loaded_of(mass, cons, lumped_ref[...])
    left = jnp.concatenate([cons, mass], axis=0)
    right = jnp.concatenate([load, cons], axis=0)
    on_diag = diagonal((half, half))
    diag = diag_ref[0].astype(F32)
    first = dot(left[:, :half], right[:, :half], (0, 0)) + jnp.where(on_diag, diag[:, :half], 0.0)
    cross = dot(left[:, :half], right[:, half:], (0, 0))
    last = dot(left[:, half:], right[:, half:], (0, 0)) + jnp.where(on_diag, diag[:, half:], 0.0)
    rows = lax.broadcasted_iota(jnp.int32, (half, half), 0)
    cols = lax.broadcasted_iota(jnp.int32, (half, half), 1)
    out_ref[0:half, 0:half] = cross.astype(BF16)
    out_ref[0:half, half:] = jnp.where(rows <= cols, first, last).astype(BF16)
    last_diag = jnp.sum(jnp.where(on_diag, last, 0.0), axis=0, keepdims=True)
    pad = jnp.concatenate([last_diag, last_diag], axis=1)
    out_ref[half : half + 8, :] = jnp.broadcast_to(pad, (8, 2 * half)).astype(BF16)
    out_ref[half + 8 :, :] = dot(modes_ref[...], load, (1, 0)).astype(BF16)


def high_kernel(
    stiff_ref, mass_ref, cons_ref, lumped_ref, modes_ref, face_ref, diag_ref, stiff_out, mass_out, coup_out
):
    cons = cons_ref[...]
    mass = mass_ref[...]
    width = cons.shape[1]
    stiff_out[0] = stiff_of(stiff_ref[...], cons, face_ref[0])
    load = loaded_of(mass, cons, lumped_ref[...])
    left = jnp.concatenate([cons, mass], axis=0)
    right = jnp.concatenate([load, cons], axis=0)
    diag = jnp.where(diagonal((width, width)), diag_ref[0].astype(F32), 0.0)
    mass_out[0] = (diag + dot(left, right, (0, 0))).astype(BF16)
    coup_out[0] = dot(modes_ref[...], load, (1, 0)).astype(BF16)


def select_rows(map_row):
    width = map_row.shape[1]
    wanted = across(column(map_row), width)
    return jnp.where(wanted == lax.broadcasted_iota(jnp.int32, (width, width), 1), 1.0, 0.0).astype(BF16)


def select_cols(map_row):
    width = map_row.shape[1]
    have = lax.broadcasted_iota(jnp.int32, (width, width), 0)
    return jnp.where(have == map_row, 1.0, 0.0).astype(BF16)


def add_stiff_kernel(map_ref, got_ref, own_ref, out_ref):
    map_row = map_ref[0]
    halfway = dot(got_ref[...], select_cols(map_row), (1, 0)).astype(BF16)
    moved = dot(select_rows(map_row), halfway, (1, 0))
    out_ref[0] = (own_ref[0].astype(F32) + moved).astype(BF16)


def add_mass_kernel(map_ref, got_ref, own_ref, coup_ref, *rest):
    mass_out, coup_out = rest[-2:]
    map_row = map_ref[0]
    width = map_row.shape[1]
    half = width // 2
    modes = coup_ref.shape[1]
    to_cols = select_cols(map_row)
    coup_out[0, 0:modes, :] = coup_ref[0]
    coup_out[0, modes:, :] = dot(got_ref[half + 8 :, :], to_cols, (1, 0)).astype(BF16)
    cross = got_ref[0:half, 0:half]
    packed = got_ref[0:half, half:].astype(F32)
    last_diag = got_ref[half : half + 8, :].astype(F32)[0:1, 0:half]
    rows = lax.broadcasted_iota(jnp.int32, (half, half), 0)
    cols = lax.broadcasted_iota(jnp.int32, (half, half), 1)
    first = jnp.where(rows < cols, packed, jnp.where(rows == cols, 0.5 * packed, 0.0)).astype(BF16)
    last = jnp.where(rows > cols, packed, jnp.where(rows == cols, 0.5 * last_diag, 0.0)).astype(BF16)
    upper = jnp.concatenate(
        [
            jnp.concatenate([first, cross], axis=1),
            jnp.concatenate([jnp.zeros_like(cross), last], axis=1),
        ],
        axis=0,
    )
    to_rows = select_rows(map_row)
    halfway = (dot(to_rows, upper, (1, 0)) + dot(to_rows, upper, (1, 1))).astype(BF16)
    mass_out[0] = (own_ref[0].astype(F32) + dot(halfway, to_cols, (1, 0))).astype(BF16)


def spec(shape, *at):
    return pl.BlockSpec(shape, lambda step: at)


def call(kernel, name, in_specs, out_specs, out_shape, flops, **extra):
    return pl.pallas_call(
        kernel,
        name=name,
        grid=(1,),
        in_specs=in_specs,
        out_specs=out_specs,
        out_shape=out_shape,
        cost_estimate=pl.CostEstimate(flops=flops, bytes_accessed=2**20, transcendentals=0),
        **extra,
    )


def local(constraint, stiff_ib, mass_ib, mass_ii, modes, stiff_faces, mass_faces, dof_map):
    cons = constraint[0, 0, 0]
    stiff = stiff_ib[0, 0, 0]
    mass = mass_ib[0, 0, 0]
    lumped = mass_ii[0, 0]
    modes = modes[0, 0, 0]
    faces = stiff_faces[0, 0, 0]
    diags = mass_faces[0, 0, 0][:, None, :]
    maps = dof_map[0, 0, 0][:, None, :]
    inner, _ = cons.shape
    width = faces.shape[-1]
    count = modes.shape[0]
    half = width // 2
    low_rows = half + 8 + count
    flat = jax.ShapeDtypeStruct

    def cols(face):
        return spec((inner, width), 0, face)

    def low_stiff(axis):
        face = 2 * axis
        return call(
            low_stiff_kernel,
            "low_stiff",
            [cols(face), cols(face), spec((1, width, width), face, 0, 0)],
            spec((width, width), 0, 0),
            flat((width, width), BF16),
            2 * inner * width * width,
        )(stiff, cons, faces)

    def low_mass(axis):
        face = 2 * axis
        return call(
            low_mass_kernel,
            "low_mass",
            [
                cols(face),
                cols(face),
                spec((1, inner), 0, 0),
                spec((count, inner), 0, 0),
                spec((1, 1, width), face, 0, 0),
            ],
            spec((low_rows, width), 0, 0),
            flat((low_rows, width), BF16),
            4 * inner * width * width,
        )(cons, mass, lumped, modes, diags)

    def high():
        def per(shape, index):
            return pl.BlockSpec(shape, index)

        return pl.pallas_call(
            high_kernel,
            name="high",
            grid=(3,),
            in_specs=[
                per((inner, width), lambda a: (0, 2 * a + 1)),
                per((inner, width), lambda a: (0, 2 * a + 1)),
                per((inner, width), lambda a: (0, 2 * a + 1)),
                per((1, inner), lambda a: (0, 0)),
                per((count, inner), lambda a: (0, 0)),
                per((1, width, width), lambda a: (2 * a + 1, 0, 0)),
                per((1, 1, width), lambda a: (2 * a + 1, 0, 0)),
            ],
            out_specs=[
                per((1, width, width), lambda a: (a, 0, 0)),
                per((1, width, width), lambda a: (a, 0, 0)),
                per((1, count, width), lambda a: (a, 0, 0)),
            ],
            out_shape=[
                flat((3, width, width), BF16),
                flat((3, width, width), BF16),
                flat((3, count, width), BF16),
            ],
            cost_estimate=pl.CostEstimate(
                flops=3 * 7 * inner * width * width, bytes_accessed=2**22, transcendentals=0
            ),
        )(stiff, mass, cons, lumped, modes, faces, diags)

    def add_stiff(axis, got, out):
        block = spec((1, width, width), axis, 0, 0)
        return call(
            add_stiff_kernel,
            "add_stiff",
            [spec((1, 1, width), axis, 0, 0), spec((width, width), 0, 0), block],
            block,
            flat((3, width, width), BF16),
            4 * width**3,
            input_output_aliases={2: 0},
        )(maps, got, out)

    def add_mass(axis, got, out, coup_own, coup_out):
        block = spec((1, width, width), axis, 0, 0)
        base = () if coup_out is None else (coup_out,)
        return call(
            add_mass_kernel,
            "add_mass",
            [
                spec((1, 1, width), axis, 0, 0),
                spec((low_rows, width), 0, 0),
                block,
                spec((1, count, width), axis, 0, 0),
                *(pl.BlockSpec(memory_space=pl.ANY) for _ in base),
            ],
            [block, spec((1, 2 * count, width), axis, 0, 0)],
            [flat((3, width, width), BF16), flat((3, 2 * count, width), BF16)],
            8 * width**3,
            input_output_aliases={2: 0, 4: 1} if base else {2: 0},
        )(maps, got, out, coup_own, *base)

    names = ("gx", "gy", "gz")
    stiff_got = {}
    mass_got = {}
    for axis in (0, 1):
        stiff_got[axis] = shifted(low_stiff(axis), names[axis])
    for axis in (0, 1):
        mass_got[axis] = shifted(low_mass(axis), names[axis])
    stiff_got[2] = shifted(low_stiff(2), names[2])
    mass_got[2] = shifted(low_mass(2), names[2])
    stiff_out, mass_out, coup_own = high()
    coup_out = None
    for axis in (2, 0, 1):
        stiff_out = add_stiff(axis, stiff_got[axis], stiff_out)
    for axis in (2, 0, 1):
        mass_out, coup_out = add_mass(axis, mass_got[axis], mass_out, coup_own, coup_out)
    outs = (stiff_out, mass_out, coup_out)
    return tuple(x[None, None, None] for x in outs)


def solution(mesh):
    tail4 = P("gx", "gy", "gz", None)
    tail5 = P("gx", "gy", "gz", None, None)
    tail6 = P("gx", "gy", "gz", None, None, None)
    placed = (tail5, tail5, tail5, tail4, tail5, tail6, tail5, tail5)
    return jax.shard_map(
        local, mesh=mesh, in_specs=placed, out_specs=(tail6, tail6, tail6), check_vma=False
    )
```
